32 devices in a mesh: gx: 4 (over y, x), gy: 4 (over z), gz: 2 (over core).
Axes of the slice: x: 2, y: 2, z: 4, core: 2. Of those that a mesh axis runs over, the one named last changes fastest.
Arguments:
- rhs_coarse: bfloat16 [32, 32, 128], P('gx'), may hold values from -24 to 24
- rhs_mid: bfloat16 [64, 64, 256], P('gx', 'gy'), may hold values from -24 to 24
- rhs_fine: bfloat16 [128, 128, 512], P('gx', 'gy', 'gz'), may hold values from -24 to 24
- occupied_coarse: int32 [4, 4, 16], P('gx'), may hold values 0 or 1
- occupied_mid: int32 [8, 8, 32], P('gx', 'gy'), may hold values 0 or 1
- occupied_fine: int32 [16, 16, 64], P('gx', 'gy', 'gz'), may hold values 0 or 1
- screen_weight: float32 [3], replicated, may hold values from 0.2 to 2
Outputs:
- solution_coarse: float32 [32, 32, 128], P('gx')
- solution_mid: float32 [64, 64, 256], P('gx', 'gy')
- solution_fine: float32 [128, 128, 512], P('gx', 'gy', 'gz')
The draws below stay inside these ranges and needn't reach their ends.
All inputs are finite; a program needn't handle non-finite values. No bound on the sum of `occupied_coarse` or of `occupied_mid` or of `occupied_fine` on one device may be relied on, other than what follows from the above.
Results may differ from the reference program's by a relative error of at most 0.0003.
Values sent between devices are 32-bit elements; how exact they have to be, the bound alone decides.
A program may use at most 128 MiB of HBM per device.

```python
import math
import jax
import jax.numpy as jnp
from jax import lax

BRICK = 8
CG_ITERS = 2
NX = 128
NY = 128
NZ = 512


def place_ends(drawn, key, least, top_value):
    shape = drawn.shape
    place = [jax.random.randint(jax.random.fold_in(key, axis), (), 0, shape[axis]) for axis in range(len(shape))]
    drawn = drawn.at[tuple(place)].set(least)
    longest = shape.index(max(shape))
    place[longest] = (place[longest] + 1) % shape[longest]
    return drawn.at[tuple(place)].set(top_value)


def shard_levels(key, extent, split, smallest, top_value):
    loudness = 1.0
    for dim, parts in split:
        heights = jax.random.uniform(jax.random.fold_in(jax.random.fold_in(key, 6), dim), (parts,), jnp.float32, smallest / len(split), top_value / len(split))
        loudness = loudness * jnp.repeat(jnp.exp(heights), extent[dim] // parts).reshape((-1,) + (1,) * (len(extent) - 1 - dim))
    return loudness


def centred(own_key, extent, deviation, bound, cuts=(), kind=jnp.bfloat16):
    loudness = shard_levels(own_key, extent, cuts, -0.22, 0.18) if cuts else 1.0
    values = jax.random.normal(own_key, extent, jnp.float32) * deviation * loudness
    return jnp.minimum(jnp.maximum(values, -bound), bound).astype(kind)


def setup_inputs(seed: int = 0) -> dict:
    arg_keys = jax.random.split(jax.random.key(seed), 8)
    rhs_coarse = centred(arg_keys[0], (NX // 4, NY // 4, NZ // 4), 4.0, 24.0, ((0, 4),))
    rhs_mid = centred(arg_keys[1], (NX // 2, NY // 2, NZ // 2), 4.0, 24.0, ((0, 4), (1, 4)))
    rhs_fine = centred(arg_keys[2], (NX, NY, NZ), 4.0, 24.0, ((0, 4), (1, 4), (2, 2)))
    occupied_coarse = place_ends((jax.random.randint(arg_keys[3], (NX // (4 * BRICK), NY // (4 * BRICK), NZ // (4 * BRICK)), 0, 2) < 1).astype(jnp.int32), jax.random.fold_in(arg_keys[3], 1), 0, 1)
    occupied_mid = place_ends((jax.random.randint(arg_keys[4], (NX // (2 * BRICK), NY // (2 * BRICK), NZ // (2 * BRICK)), 0, 2) < 1).astype(jnp.int32), jax.random.fold_in(arg_keys[4], 1), 0, 1)
    occupied_fine = place_ends((jax.random.randint(arg_keys[5], (NX // BRICK, NY // BRICK, NZ // BRICK), 0, 2) < 1).astype(jnp.int32), jax.random.fold_in(arg_keys[5], 1), 0, 1)
    screen_weight = jnp.clip(jnp.exp(jax.random.uniform(arg_keys[6], (3,), jnp.float32, math.log(0.2), math.log(2.0))), 0.2, 2.0)
    return {"rhs_coarse": rhs_coarse, "rhs_mid": rhs_mid, "rhs_fine": rhs_fine, "occupied_coarse": occupied_coarse, "occupied_mid": occupied_mid, "occupied_fine": occupied_fine, "screen_weight": screen_weight}


def alternate(even_cells, odd_cells, dim_index):
    stacked = jnp.stack([even_cells, odd_cells], axis=dim_index + 1)
    new_shape = list(even_cells.shape)
    new_shape[dim_index] = new_shape[dim_index] * 2
    return stacked.reshape(new_shape)


def prolong_axis(padded, dim_index, extend):
    length = padded.shape[dim_index]
    below_cells = lax.slice_in_dim(padded, 0, length - 2, axis=dim_index)
    middle = lax.slice_in_dim(padded, 1, length - 1, axis=dim_index)
    above_cells = lax.slice_in_dim(padded, 2, length, axis=dim_index)
    refined = alternate(0.75 * middle + 0.25 * below_cells, 0.75 * middle + 0.25 * above_cells, dim_index)
    if extend:
        first_rim = 0.75 * lax.slice_in_dim(padded, 0, 1, axis=dim_index) + 0.25 * lax.slice_in_dim(padded, 1, 2, axis=dim_index)
        last_rim = 0.75 * lax.slice_in_dim(padded, length - 1, length, axis=dim_index) + 0.25 * lax.slice_in_dim(padded, length - 2, length - 1, axis=dim_index)
        refined = jnp.concatenate([first_rim, refined, last_rim], axis=dim_index)
    return refined


def prolong(coarse):
    padded = jnp.pad(coarse, 1)
    for dim_index in range(3):
        padded = prolong_axis(padded, dim_index, False)
    return padded


def screening(occupied, weight):
    brick_flags = occupied.astype(jnp.float32)
    brick_shape = occupied.shape
    spread = jnp.broadcast_to(brick_flags[:, None, :, None, :, None], (brick_shape[0], BRICK, brick_shape[1], BRICK, brick_shape[2], BRICK))
    cell_flags = spread.reshape(brick_shape[0] * BRICK, brick_shape[1] * BRICK, brick_shape[2] * BRICK)
    return weight * (0.25 + cell_flags)


def stencil(padded, screen):
    centre = padded[1:-1, 1:-1, 1:-1]
    beside = padded[2:, 1:-1, 1:-1] + padded[:-2, 1:-1, 1:-1]
    beside = beside + padded[1:-1, 2:, 1:-1] + padded[1:-1, :-2, 1:-1]
    beside = beside + padded[1:-1, 1:-1, 2:] + padded[1:-1, 1:-1, :-2]
    return (6.0 + screen) * centre - beside


def cg_solve(right_side, guess, screen):
    target = right_side.astype(jnp.float32)
    iterate = guess
    residual = target - stencil(jnp.pad(iterate, 1), screen)
    direction = residual
    norm_now = jnp.sum(residual * residual)
    for turn_index in range(CG_ITERS):
        image = stencil(jnp.pad(direction, 1), screen)
        step_size = norm_now / jnp.sum(direction * image)
        iterate = iterate + step_size * direction
        residual = residual - step_size * image
        if turn_index + 1 < CG_ITERS:
            norm_next = jnp.sum(residual * residual)
            direction = residual + (norm_next / norm_now) * direction
            norm_now = norm_next
    return iterate


def reference(rhs_coarse, rhs_mid, rhs_fine, occupied_coarse, occupied_mid, occupied_fine, screen_weight):
    start_guess = jnp.zeros(rhs_coarse.shape, jnp.float32)
    solution_coarse = cg_solve(rhs_coarse, start_guess, screening(occupied_coarse, screen_weight[0]))
    solution_mid = cg_solve(rhs_mid, prolong(solution_coarse), screening(occupied_mid, screen_weight[1]))
    solution_fine = cg_solve(rhs_fine, prolong(solution_mid), screening(occupied_fine, screen_weight[2]))
    return solution_coarse, solution_mid, solution_fine
```

```python
import functools

import jax
import jax.numpy as jnp
from jax import lax
from jax.experimental import pallas as pl
from jax.experimental.pallas import tpu as pltpu
from jax.sharding import PartitionSpec as P

MESH = pl.DeviceIdType.MESH
F32 = jnp.float32
BF16 = jnp.bfloat16
PAD = 4
ROWS = 8
LANES = 128


def iota(shape, dim):
    return lax.broadcasted_iota(jnp.int32, shape, dim)


def logical(index, own, extra):
    if extra == 0:
        return index
    return jnp.where(index < own + extra // 2, index, index - (own + extra))


def prolong_matrix(fine, coarse, total, fine_dim):
    base = lax.shift_right_arithmetic(fine, 1)
    beside = base + 2 * (fine & 1) - 1
    inside = jnp.logical_and(fine >= 0, fine < total)
    value = jnp.where(coarse == base, 0.75, jnp.where(coarse == beside, 0.25, 0.0))
    return jnp.where(inside, value, 0.0).astype(BF16)


def split(values):
    high = values.astype(BF16)
    return high, (values - high.astype(F32)).astype(BF16)


def mm(a, b):
    return jnp.dot(a, b, preferred_element_type=F32)


def fold_rows(values):
    total = values[0:ROWS]
    for row in range(ROWS, values.shape[0], ROWS):
        total = total + values[row : row + ROWS]
    out = total[:, 0:LANES]
    for lane in range(LANES, values.shape[1], LANES):
        out = out + total[:, lane : lane + LANES]
    return out


def coefficients(m0, n1, n2, n3):
    rho = n1 / m0
    spread = n2 - rho * n1
    bent = 6.0 * spread + (n3 - 2.0 * rho * n2 + rho * rho * n1)
    turn = jnp.where(bent > 0.0, jnp.maximum(spread, 0.0) / bent, 0.0)
    first = m0 / ((6.0 + rho) * m0 - jnp.maximum(spread, 0.0) * turn)
    second = -first * turn
    return first - second * rho, second


def kernel(
    dims,
    rhs_c, rhs_m, rhs_f, occ_c, occ_m, occ_f, weight,
    out_c, out_m, out_f,
    cr, cw, cs, cx, ctz, ct, oc,
    mb, mg, mr, mw, ms, mx, mtz, mt, om, m_up, m_dn, m_fu, m_fd, om_l, om_r,
    fb, fg, fr, fw, fs, of, f_up, f_dn, f_fu, f_fd, of_l, of_r,
    am, af, ss, rs, sm, rm, sf, rf,
):
    nx, ny, nz = dims
    ix, iy, iz = lax.axis_index("gx"), lax.axis_index("gy"), lax.axis_index("gz")
    xc, yc, zc = rhs_c.shape
    xm, ym, zm = rhs_m.shape
    xf, yf, zf = rhs_f.shape
    bc, bm, bf = occ_c.shape, occ_m.shape, occ_f.shape
    total_xc = xc * nx
    x_low, x_high = ix > 0, ix < nx - 1
    y_low, y_high = iy > 0, iy < ny - 1

    for ref in (om, of):
        ref[...] = jnp.zeros_like(ref)
    own_x = pl.ds(ix * xc + 3, xc)
    own_bx = pl.ds(ix * bc[0], bc[0])
    cr[own_x] = rhs_c[...].astype(F32)
    oc[own_bx] = jnp.zeros((bc[0],) + tuple(oc.shape[1:]), F32)
    oc[own_bx, 0 : bc[1], 0 : bc[2]] = occ_c[...].astype(F32)
    om[1 : 1 + bm[0], 0 : bm[1], 0 : bm[2]] = occ_m[...].astype(F32)
    of[1 : 1 + bf[0], 0 : bf[1], 0 : bf[2]] = occ_f[...].astype(F32)
    mb[PAD : PAD + xm, 0:ym, :] = rhs_m[...].astype(F32)

    def fill_fine(x, carry):
        fb[x + PAD, 0:yf, 0:zf] = rhs_f[x].astype(F32)
        return carry

    lax.fori_loop(0, xf, fill_fine, 0)

    barrier = pltpu.get_barrier_semaphore()
    peers = [(a, b, c) for a in range(nx) for b in range(ny) for c in range(nz)][1:]

    def at(offset):
        return (
            lax.rem(ix + offset[0], nx), lax.rem(iy + offset[1], ny), lax.rem(iz + offset[2], nz)
        )

    for offset in peers:
        pl.semaphore_signal(barrier, inc=1, device_id=at(offset), device_id_type=MESH)

    zero_c = jnp.zeros((3, yc, zc), F32)
    cr[0:3] = zero_c
    cr[total_xc + 3 : total_xc + 6] = zero_c
    cw[0:3] = zero_c
    cw[total_xc + 3 : total_xc + 6] = zero_c

    @pl.when(jnp.logical_not(x_low))
    def _():
        mb[1:4, 0:ym, :] = jnp.zeros((3, ym, zm), F32)
        fb[2:4, 0:yf, :] = jnp.zeros((2, yf, fb.shape[2]), F32)

    @pl.when(jnp.logical_not(x_high))
    def _():
        mb[PAD + xm : PAD + xm + 3, 0:ym, :] = jnp.zeros((3, ym, zm), F32)
        fb[PAD + xf : PAD + xf + 2, 0:yf, :] = jnp.zeros((2, yf, fb.shape[2]), F32)

    @pl.when(jnp.logical_not(y_low))
    def _():
        for ref in (m_fu, f_fu, om_l, of_l):
            ref[...] = jnp.zeros_like(ref)

    @pl.when(jnp.logical_not(y_high))
    def _():
        for ref in (m_fd, f_fd, om_r, of_r):
            ref[...] = jnp.zeros_like(ref)

    pl.semaphore_wait(barrier, len(peers))

    used = [0]

    def copy(src, dst, target):
        k = used[0]
        used[0] += 1
        return pltpu.make_async_remote_copy(
            src_ref=src, dst_ref=dst, send_sem=ss.at[k], recv_sem=rs.at[k],
            device_id=target, device_id_type=MESH,
        )

    sends = []

    def start(items):
        for c, can_send, _ in items:
            if can_send is None:
                c.start()
            else:
                pl.when(can_send)(c.start)
        sends.extend(items)

    def arrive(items):
        for c, _, can_recv in items:
            if can_recv is None:
                c.wait_recv()
            else:
                pl.when(can_recv)(c.wait_recv)

    def left(items):
        for c, can_send, _ in items:
            if can_send is None:
                c.wait_send()
            else:
                pl.when(can_send)(c.wait_send)

    gather = []
    for d in range(1, nx):
        target = {"gx": lax.rem(ix + d, nx)}
        gather.append((d, copy(cr.at[own_x], cr.at[own_x], target), None))
        gather.append((d, copy(oc.at[own_bx], oc.at[own_bx], target), None))
    for _, c, _ in gather:
        c.start()
    z_fine = []
    if nz == 2:
        target = {"gz": 1 - iz}
        low = pl.ds(pl.multiple_of((1 - iz) * (zf - LANES), LANES), LANES)
        z_fine.append((copy(
            fb.at[PAD : PAD + xf, 0:yf, low],
            fb.at[PAD : PAD + xf, 0:yf, zf : zf + LANES], target), None, None))
        z_fine.append((copy(
            of.at[1 : 1 + bf[0], :, 0:LANES], of.at[1 : 1 + bf[0], :, LANES : 2 * LANES],
            target), None, None))
    else:
        fb[PAD : PAD + xf, 0:yf, zf:] = jnp.zeros((xf, yf, LANES), F32)
    start(z_fine)

    def x_swap(ref, occ, own, rows, width, bricks):
        items = []
        up, down = {"gx": ix + 1}, {"gx": ix - 1}
        items.append((copy(ref.at[PAD + own - width : PAD + own, 0:rows, :],
                           ref.at[PAD - width : PAD, 0:rows, :], up), x_high, x_low))
        items.append((copy(ref.at[PAD : PAD + width, 0:rows, :],
                           ref.at[PAD + own : PAD + own + width, 0:rows, :], down), x_low, x_high))
        items.append((copy(occ.at[bricks], occ.at[0], up), x_high, x_low))
        items.append((copy(occ.at[1], occ.at[bricks + 1], down), x_low, x_high))
        return items

    def y_swap(ref, occ, own, width, to_up, to_down, from_low, from_high, occ_l, occ_r, planes):
        first, count = planes
        to_up[...] = ref[first : first + count, own - width : own, :]
        to_down[...] = ref[first : first + count, 0:width, :]
        up, down = {"gy": iy + 1}, {"gy": iy - 1}
        return [
            (copy(to_up, from_low, up), y_high, y_low),
            (copy(to_down, from_high, down), y_low, y_high),
            (copy(occ, occ_l, up), y_high, y_low),
            (copy(occ, occ_r, down), y_low, y_high),
        ]

    def y_merge(ref, own, width, from_low, from_high, planes):
        first, count = planes
        parts = [from_high[...], from_low[...]]
        if 2 * width < ROWS:
            parts.insert(1, jnp.zeros((count, ROWS - 2 * width, ref.shape[2]), F32))
        ref[first : first + count, own : own + ROWS, :] = jnp.concatenate(parts, axis=1)

    x_mid = x_swap(mb, om, xm, ym, 3, bm[0])
    start(x_mid)
    mid_planes, fine_planes = (1, xm + 6), (2, xf + 4)

    def row_prolong(own, extra, index, total, cols, col_own, col_extra, col_index):
        shape = (own + extra, cols)
        fine = logical(iota(shape, 0), own, extra) + own * index
        coarse = logical(iota(shape, 1), col_own, col_extra) + col_own * col_index
        return prolong_matrix(fine, coarse, total, 0)

    def lane_prolong(own, extra, index, total, rows):
        shape = (rows, own + extra)
        fine = logical(iota(shape, 1), own, extra) + own * index
        return prolong_matrix(fine, iota(shape, 0), total, 1)

    def screens(dest, occ_parts, own, extra_rows, bricks_y, lane_matrix, level):
        count = dest.shape[0]
        side = own // bricks_y
        cols = ROWS * len(occ_parts)
        shape = (dest.shape[1], cols)
        brick = lax.div(logical(iota(shape, 0), own, extra_rows) + side, side) - 1
        place = jnp.where(
            brick < 0, ROWS + bricks_y - 1, jnp.where(brick >= bricks_y, 2 * ROWS, brick)
        )
        row_matrix = (place == iota(shape, 1)).astype(BF16)
        for x in range(count):
            flags = jnp.concatenate([part[x] for part in occ_parts], axis=0).astype(BF16)
            wide = mm(flags, lane_matrix).astype(BF16)
            dest[x] = weight[level] * (0.25 + mm(row_matrix, wide))

    def along_y(v):
        n = v.shape[0]
        return pltpu.roll(v, 1, 0), pltpu.roll(v, n - 1, 0)

    def along_z(v):
        n = v.shape[1]
        return pltpu.roll(v, 1, 1), pltpu.roll(v, n - 1, 1)

    arrive(z_fine)
    x_fine = x_swap(fb, of, xf, yf, 2, bf[0])
    start(x_fine)
    arrive(x_mid)
    y_mid = y_swap(mb, om, ym, 4, m_up, m_dn, m_fu, m_fd, om_l, om_r, mid_planes)
    start(y_mid)
    for _, c, _ in gather:
        c.wait_recv()

    lanes_c = (iota((LANES, zc), 0) == lax.div(iota((LANES, zc), 1), zc // bc[2])).astype(BF16)
    screens(cs, [oc], yc, 0, bc[1], lanes_c, 0)
    side_c = xc // bc[0]
    shape_c = (yc, zc)
    row_c, lane_c = iota(shape_c, 0), iota(shape_c, 1)

    def sum_c(v, both):
        yu, yd = along_y(v)
        zu, zd = along_z(v)
        total = jnp.where(row_c < yc - 1, yd, 0.0) + jnp.where(lane_c < zc - 1, zd, 0.0)
        if both:
            total = total + jnp.where(row_c > 0, yu, 0.0) + jnp.where(lane_c > 0, zu, 0.0)
        return total

    def coarse_w(x, carry):
        r = cr[x + 3]
        cw[x + 3] = cs[lax.div(x, side_c)] * r - (cr[x + 2] + cr[x + 4] + sum_c(r, True))
        return carry

    lax.fori_loop(0, total_xc, coarse_w, 0)

    arrive(x_fine)
    y_fine = y_swap(fb, of, yf, 2, f_up, f_dn, f_fu, f_fd, of_l, of_r, fine_planes)
    start(y_fine)

    def coarse_moments(x, acc):
        r, w = cr[x + 3], cw[x + 3]
        image = cs[lax.div(x, side_c)] * w - 2.0 * (cw[x + 4] + sum_c(w, False))
        return tuple(a + fold_rows(b) for a, b in zip(acc, (r * r, r * w, w * w, w * image)))

    zero = jnp.zeros((ROWS, LANES), F32)

    def whole_sum(v):
        return jnp.sum(jnp.sum(v, axis=0, keepdims=True), axis=1, keepdims=True)

    acc = lax.fori_loop(0, total_xc, coarse_moments, (zero,) * 4)
    ka, kb = coefficients(*[whole_sum(a) for a in acc])
    for j in range(xc + 6):
        cx[j] = ka * cr[ix * xc + j] + kb * cw[ix * xc + j]
    out_c[...] = cx[3 : 3 + xc]

    def prolong(src, tz, dst, lane_matrix, row_matrix):
        n, rows, lanes = src.shape
        high, low = split(src[...].reshape(n * rows, lanes))
        tz[...] = (mm(high, lane_matrix) + mm(low, lane_matrix)).reshape(tz.shape)
        for j in range(n):
            high, low = split(tz[j])
            dst[j] = mm(row_matrix, high) + mm(row_matrix, low)

    def interpolate(t, g, own, first, total):
        for p in range(own + 2 * PAD):
            m = p - PAD
            j = m // 2
            beside = min(max(j + (1 if m % 2 else -1) - first, 0), t.shape[0] - 1)
            place = own * ix + m
            keep = jnp.logical_and(place >= 0, place < total).astype(F32)
            g[p] = (0.75 * keep) * t[j - first] + (0.25 * keep) * t[beside]

    def neighbours(v, low_lane, high_lane):
        yu, yd = along_y(v)
        zu, zd = along_z(v)
        if low_lane is not None:
            zu, zd = jnp.where(low_lane, 0.0, zu), jnp.where(high_lane, 0.0, zd)
        return yu + yd + zu + zd

    def later(v, high_lane):
        yd = along_y(v)[1]
        zd = along_z(v)[1]
        if high_lane is not None:
            zd = jnp.where(high_lane, 0.0, zd)
        return yd + zd

    def run_depth(b, g, r, w, s, own, rows, lanes, reach, side, ends, mask):
        low_lane, high_lane = ends
        total_x = own * nx

        def inside(p):
            place = own * ix + p - PAD
            return jnp.logical_and(place >= 0, place < total_x).astype(F32)

        def brick(p):
            return lax.div(p + (side - PAD), side)

        def make_r(p, carry):
            c = g[p]
            value = b[p] - (6.0 + s[brick(p)]) * c
            value = value + (g[p - 1] + g[p + 1]) + neighbours(c, low_lane, high_lane)
            r[p] = value * (mask * inside(p))
            return carry

        lax.fori_loop(PAD - reach, PAD + own + reach, make_r, 0)

        def make_w(p, carry):
            c = r[p]
            value = s[brick(p)] * c - (r[p - 1] + r[p + 1]) - neighbours(c, low_lane, high_lane)
            w[p] = value * (mask * inside(p))
            return carry

        lax.fori_loop(PAD - reach + 1, PAD + own + reach - 1, make_w, 0)

        def moments(p, acc):
            rv, wv = r[p, 0:rows, 0:lanes], w[p, 0:rows, 0:lanes]
            full = w[p]
            image = s[brick(p), 0:rows, 0:lanes] * wv - 2.0 * (
                w[p + 1, 0:rows, 0:lanes] + later(full, high_lane)[0:rows, 0:lanes]
            )
            return tuple(
                a + fold_rows(v) for a, v in zip(acc, (rv * rv, rv * wv, wv * wv, wv * image))
            )

        return lax.fori_loop(PAD, PAD + own, moments, (zero,) * 4)

    def exchange(acc, buf, send, recv, offsets, slot):
        parts = [jnp.sum(a, axis=0, keepdims=True) for a in acc]
        buf[slot] = jnp.concatenate(parts + [jnp.zeros((ROWS - 4, LANES), F32)], axis=0)
        copies = []
        for k, offset in enumerate(offsets):
            c = pltpu.make_async_remote_copy(
                src_ref=buf.at[slot], dst_ref=buf.at[slot], send_sem=send.at[k],
                recv_sem=recv.at[k], device_id=at(offset), device_id_type=MESH,
            )
            c.start()
            copies.append(c)
        for c in copies:
            c.wait_recv()
        total = buf[0]
        for k in range(1, buf.shape[0]):
            total = total + buf[k]
        total = jnp.sum(total, axis=1, keepdims=True)
        return coefficients(*[total[k : k + 1] for k in range(4)]), copies

    prolong(
        cx, ctz, ct, lane_prolong(zm, 0, 0, zm, zc),
        row_prolong(ym, ROWS, iy, ym * ny, yc, yc, 0, 0),
    )
    interpolate(ct, mg, xm, -3, xm * nx)
    arrive(y_mid)
    left(x_mid)
    y_merge(mb, ym, 4, m_fu, m_fd, mid_planes)
    lanes_m = (iota((LANES, zm), 0) == lax.div(iota((LANES, zm), 1), zm // bm[2])).astype(BF16)
    screens(ms, [om, om_l, om_r], ym, ROWS, bm[1], lanes_m, 1)
    shape_m = (ym + ROWS, zm)
    row_m = logical(iota(shape_m, 0), ym, ROWS) + ym * iy
    mask_m = jnp.logical_and(row_m >= 0, row_m < ym * ny).astype(F32)
    ends_m = (iota(shape_m, 1) == 0, iota(shape_m, 1) == zm - 1)
    acc = run_depth(mb, mg, mr, mw, ms, xm, ym, zm, 3, xm // bm[0], ends_m, mask_m)
    flat = [o for o in peers if o[2] == 0]
    (ka, kb), mid_copies = exchange(acc, am, sm, rm, flat, ix * ny + iy)
    for p in range(2, xm + 6):
        value = mg[p] + ka * mr[p] + kb * mw[p]
        mx[p - 2] = value
        if PAD <= p < PAD + xm:
            out_m[p - PAD] = value[0:ym]

    prolong(
        mx, mtz, mt, lane_prolong(zf, LANES, iz, zf * nz, zm),
        row_prolong(yf, ROWS, iy, yf * ny, ym + ROWS, ym, ROWS, iy),
    )
    interpolate(mt, fg, xf, -2, xf * nx)
    arrive(y_fine)
    left(x_fine)
    left(z_fine)
    y_merge(fb, yf, 2, f_fu, f_fd, fine_planes)
    shape_e = (2 * LANES, zf + LANES)
    cell = logical(iota(shape_e, 1), zf, LANES)
    side_z = zf // bf[2]
    brick = lax.div(cell + side_z * LANES, side_z) - LANES
    place = jnp.where(
        brick < 0, LANES + bf[2] + brick, jnp.where(brick >= bf[2], LANES + brick - bf[2], brick)
    )
    lanes_f = (place == iota(shape_e, 0)).astype(BF16)
    screens(fs, [of, of_l, of_r], yf, ROWS, bf[1], lanes_f, 2)
    shape_f = (yf + ROWS, zf + LANES)
    row_f = logical(iota(shape_f, 0), yf, ROWS) + yf * iy
    lane_f = logical(iota(shape_f, 1), zf, LANES) + zf * iz
    mask_f = jnp.logical_and(
        jnp.logical_and(row_f >= 0, row_f < yf * ny), jnp.logical_and(lane_f >= 0, lane_f < zf * nz)
    ).astype(F32)
    acc = run_depth(fb, fg, fr, fw, fs, xf, yf, zf, 2, xf // bf[0], (None, None), mask_f)
    (ka, kb), fine_copies = exchange(acc, af, sf, rf, peers, (ix * ny + iy) * nz + iz)

    def finish(x, carry):
        p = x + PAD
        out_f[x] = (
            fg[p, 0:yf, 0:zf] + ka * fr[p, 0:yf, 0:zf] + kb * fw[p, 0:yf, 0:zf]
        )
        return carry

    lax.fori_loop(0, xf, finish, 0)

    for _, c, _ in gather:
        c.wait_send()
    left(not_in(sends, x_mid + x_fine + z_fine))
    for c in mid_copies + fine_copies:
        c.wait_send()


def not_in(items, waited):
    done = [id(item) for item in waited]
    return [item for item in items if id(item) not in done]


def shards(dims, *args):
    nx, ny, nz = dims
    rhs_c, rhs_m, rhs_f, occ_c, occ_m, occ_f, _ = args
    xc, yc, zc = rhs_c.shape
    xm, ym, zm = rhs_m.shape
    xf, yf, zf = rhs_f.shape
    me, fe = (ym + ROWS, zm), (yf + ROWS, zf + LANES)

    def buf(*shape):
        return pltpu.VMEM(shape, F32)

    bm, bf = occ_m.shape[0] + 2, occ_f.shape[0] + 2
    scratch = [
        buf(xc * nx + 6, yc, zc), buf(xc * nx + 6, yc, zc), buf(occ_c.shape[0] * nx, yc, zc),
        buf(xc + 6, yc, zc), buf(xc + 6, yc, zm), buf(xc + 6, *me),
        buf(occ_c.shape[0] * nx, ROWS, LANES),
        buf(xm + 8, *me), buf(xm + 8, *me), buf(xm + 8, *me), buf(xm + 8, *me), buf(bm, *me),
        buf(xm + 4, *me), buf(xm + 4, me[0], fe[1]), buf(xm + 4, *fe),
        buf(bm, ROWS, LANES),
        buf(xm + 6, 4, zm), buf(xm + 6, 4, zm), buf(xm + 6, 4, zm), buf(xm + 6, 4, zm),
        buf(bm, ROWS, LANES), buf(bm, ROWS, LANES),
        buf(xf + 8, *fe), buf(xf + 8, *fe), buf(xf + 8, *fe), buf(xf + 8, *fe), buf(bf, *fe),
        buf(bf, ROWS, 2 * LANES),
        buf(xf + 4, 2, fe[1]), buf(xf + 4, 2, fe[1]), buf(xf + 4, 2, fe[1]), buf(xf + 4, 2, fe[1]),
        buf(bf, ROWS, 2 * LANES), buf(bf, ROWS, 2 * LANES),
        buf(nx * ny, ROWS, LANES), buf(nx * ny * nz, ROWS, LANES),
        pltpu.SemaphoreType.DMA((2 * nx + 16,)), pltpu.SemaphoreType.DMA((2 * nx + 16,)),
        pltpu.SemaphoreType.DMA((nx * ny,)), pltpu.SemaphoreType.DMA((nx * ny,)),
        pltpu.SemaphoreType.DMA((nx * ny * nz,)), pltpu.SemaphoreType.DMA((nx * ny * nz,)),
    ]
    vmem = pl.BlockSpec(memory_space=pltpu.VMEM)
    return pl.pallas_call(
        functools.partial(kernel, dims),
        out_shape=[jax.ShapeDtypeStruct(a.shape, F32) for a in args[:3]],
        in_specs=[vmem] * 6 + [pl.BlockSpec(memory_space=pltpu.SMEM)],
        out_specs=[vmem] * 3,
        scratch_shapes=scratch,
        compiler_params=pltpu.CompilerParams(
            collective_id=0, has_side_effects=True, vmem_limit_bytes=60 * 1024 * 1024
        ),
    )(*args)


def solution(mesh):
    dims = tuple(mesh.shape[axis] for axis in ("gx", "gy", "gz"))
    in_specs = (
        P("gx", None, None), P("gx", "gy", None), P("gx", "gy", "gz"),
        P("gx", None, None), P("gx", "gy", None), P("gx", "gy", "gz"), P(),
    )
    out_specs = (P("gx", None, None), P("gx", "gy", None), P("gx", "gy", "gz"))
    return jax.shard_map(
        functools.partial(shards, dims), mesh=mesh, in_specs=in_specs, out_specs=out_specs,
        check_vma=False,
    )
```

```python
import functools

import jax
import jax.numpy as jnp
from jax import lax
from jax.experimental import pallas as pl
from jax.experimental.pallas import tpu as pltpu
from jax.sharding import PartitionSpec as P

MESH = pl.DeviceIdType.MESH
F32 = jnp.float32
BF16 = jnp.bfloat16
PAD = 4
ROWS = 8
LANES = 128


def iota(shape, dim):
    return lax.broadcasted_iota(jnp.int32, shape, dim)


def logical(index, own, extra):
    if extra == 0:
        return index
    return jnp.where(index < own + extra // 2, index, index - (own + extra))


def prolong_matrix(fine, coarse, total, fine_dim):
    base = lax.shift_right_arithmetic(fine, 1)
    beside = base + 2 * (fine & 1) - 1
    inside = jnp.logical_and(fine >= 0, fine < total)
    value = jnp.where(coarse == base, 0.75, jnp.where(coarse == beside, 0.25, 0.0))
    return jnp.where(inside, value, 0.0).astype(BF16)


def split(values):
    high = values.astype(BF16)
    return high, (values - high.astype(F32)).astype(BF16)


def mm(a, b):
    return jnp.dot(a, b, preferred_element_type=F32)


def fold_rows(values):
    total = values[0:ROWS]
    for row in range(ROWS, values.shape[0], ROWS):
        total = total + values[row : row + ROWS]
    out = total[:, 0:LANES]
    for lane in range(LANES, values.shape[1], LANES):
        out = out + total[:, lane : lane + LANES]
    return out


def coefficients(m0, n1, n2, n3):
    rho = n1 / m0
    spread = n2 - rho * n1
    bent = 6.0 * spread + (n3 - 2.0 * rho * n2 + rho * rho * n1)
    turn = jnp.where(bent > 0.0, jnp.maximum(spread, 0.0) / bent, 0.0)
    first = m0 / ((6.0 + rho) * m0 - jnp.maximum(spread, 0.0) * turn)
    second = -first * turn
    return first - second * rho, second


def kernel(
    dims,
    rhs_c, rhs_m, rhs_f, occ_c, occ_m, occ_f, weight,
    out_c, out_m, out_f,
    cr, cw, cs, cx, ctz, ct, oc,
    mb, mg, mr, mw, ms, mx, mtz, mt, om, m_up, m_dn, m_fu, m_fd, om_l, om_r,
    fb, fg, fr, fw, fs, of, f_up, f_dn, f_fu, f_fd, of_l, of_r,
    ac, am, af, ag, ss, rs, sc, rc, sm, rm, sf, rf, sg, rg,
):
    nx, ny, nz = dims
    ix, iy, iz = lax.axis_index("gx"), lax.axis_index("gy"), lax.axis_index("gz")
    xc, yc, zc = rhs_c.shape
    xm, ym, zm = rhs_m.shape
    xf, yf, zf = rhs_f.shape
    bc, bm, bf = occ_c.shape, occ_m.shape, occ_f.shape
    x_low, x_high = ix > 0, ix < nx - 1
    y_low, y_high = iy > 0, iy < ny - 1

    for ref in (oc, om, of):
        ref[...] = jnp.zeros_like(ref)
    cr[PAD : PAD + xc] = rhs_c[...].astype(F32)
    oc[1 : 1 + bc[0], 0 : bc[1], 0 : bc[2]] = occ_c[...].astype(F32)
    om[1 : 1 + bm[0], 0 : bm[1], 0 : bm[2]] = occ_m[...].astype(F32)
    of[1 : 1 + bf[0], 0 : bf[1], 0 : bf[2]] = occ_f[...].astype(F32)
    mb[PAD : PAD + xm, 0:ym, :] = rhs_m[...].astype(F32)

    def fill_fine(x, carry):
        fb[x + PAD, 0:yf, 0:zf] = rhs_f[x].astype(F32)
        return carry

    lax.fori_loop(0, xf, fill_fine, 0)

    barrier = pltpu.get_barrier_semaphore()
    flat = [(a, b, 0) for a in range(nx) for b in range(ny)][1:]
    across = [(0, 0, c) for c in range(1, nz)]
    peers = flat + across

    def at(offset):
        return (
            lax.rem(ix + offset[0], nx), lax.rem(iy + offset[1], ny), lax.rem(iz + offset[2], nz)
        )

    for offset in peers:
        pl.semaphore_signal(barrier, inc=1, device_id=at(offset), device_id_type=MESH)

    @pl.when(jnp.logical_not(x_low))
    def _():
        cr[0:4] = jnp.zeros((4, yc, zc), F32)
        mb[1:4, 0:ym, :] = jnp.zeros((3, ym, zm), F32)
        fb[2:4, 0:yf, :] = jnp.zeros((2, yf, fb.shape[2]), F32)

    @pl.when(jnp.logical_not(x_high))
    def _():
        cr[PAD + xc : PAD + xc + 4] = jnp.zeros((4, yc, zc), F32)
        mb[PAD + xm : PAD + xm + 3, 0:ym, :] = jnp.zeros((3, ym, zm), F32)
        fb[PAD + xf : PAD + xf + 2, 0:yf, :] = jnp.zeros((2, yf, fb.shape[2]), F32)

    @pl.when(jnp.logical_not(x_low))
    def _():
        for ref, reach in ((m_fu, 3), (m_fd, 3), (f_fu, 2), (f_fd, 2)):
            ref[0:reach] = jnp.zeros((reach,) + tuple(ref.shape[1:]), F32)
        for ref in (om_l, om_r, of_l, of_r):
            ref[0:1] = jnp.zeros((1,) + tuple(ref.shape[1:]), F32)

    @pl.when(jnp.logical_not(x_high))
    def _():
        for ref, reach in ((m_fu, 3), (m_fd, 3), (f_fu, 2), (f_fd, 2)):
            size = ref.shape[0]
            ref[size - reach : size] = jnp.zeros((reach,) + tuple(ref.shape[1:]), F32)
        for ref in (om_l, om_r, of_l, of_r):
            size = ref.shape[0]
            ref[size - 1 : size] = jnp.zeros((1,) + tuple(ref.shape[1:]), F32)

    @pl.when(jnp.logical_not(y_low))
    def _():
        for ref in (m_fu, f_fu, om_l, of_l):
            ref[...] = jnp.zeros_like(ref)

    @pl.when(jnp.logical_not(y_high))
    def _():
        for ref in (m_fd, f_fd, om_r, of_r):
            ref[...] = jnp.zeros_like(ref)

    pl.semaphore_wait(barrier, len(peers))

    used = [0]

    def copy(src, dst, target):
        k = used[0]
        used[0] += 1
        return pltpu.make_async_remote_copy(
            src_ref=src, dst_ref=dst, send_sem=ss.at[k], recv_sem=rs.at[k],
            device_id=target, device_id_type=MESH,
        )

    def start(items):
        for c, can_send, _ in items:
            if can_send is None:
                c.start()
            else:
                pl.when(can_send)(c.start)

    def arrive(items):
        for c, _, can_recv in items:
            if can_recv is None:
                c.wait_recv()
            else:
                pl.when(can_recv)(c.wait_recv)

    def left(items):
        for c, can_send, _ in items:
            if can_send is None:
                c.wait_send()
            else:
                pl.when(can_send)(c.wait_send)

    def x_swap(ref, occ, own, rows, width, bricks):
        items = []
        up, down = {"gx": ix + 1}, {"gx": ix - 1}
        items.append((copy(ref.at[PAD + own - width : PAD + own, 0:rows, :],
                           ref.at[PAD - width : PAD, 0:rows, :], up), x_high, x_low))
        items.append((copy(ref.at[PAD : PAD + width, 0:rows, :],
                           ref.at[PAD + own : PAD + own + width, 0:rows, :], down), x_low, x_high))
        items.append((copy(occ.at[bricks], occ.at[0], up), x_high, x_low))
        items.append((copy(occ.at[1], occ.at[bricks + 1], down), x_low, x_high))
        return items

    x_coarse = x_swap(cr, oc, xc, yc, 4, bc[0])
    start(x_coarse)

    def y_swap(ref, occ, own, rows, width, reach, to_up, to_down, from_low, from_high, occ_l, occ_r, bricks):
        planes, flags = pl.ds(reach, own), pl.ds(1, bricks)
        to_up[planes] = ref[PAD : PAD + own, rows - width : rows, :]
        to_down[planes] = ref[PAD : PAD + own, 0:width, :]
        items = []
        for out, dst, occ_dst, step, can_send, can_recv in (
            (to_up, from_low, occ_l, 1, y_high, y_low), (to_down, from_high, occ_r, -1, y_low, y_high)
        ):
            side = {"gy": iy + step}
            items.append((copy(out.at[planes], dst.at[planes], side), can_send, can_recv))
            items.append((copy(occ.at[flags], occ_dst.at[flags], side), can_send, can_recv))
            corner = {"gx": ix + 1, "gy": iy + step}
            when = (jnp.logical_and(can_send, x_high), jnp.logical_and(can_recv, x_low))
            items.append((copy(out.at[pl.ds(own, reach)], dst.at[pl.ds(0, reach)], corner), *when))
            items.append((copy(occ.at[bricks], occ_dst.at[0], corner), *when))
            corner = {"gx": ix - 1, "gy": iy + step}
            when = (jnp.logical_and(can_send, x_low), jnp.logical_and(can_recv, x_high))
            items.append(
                (copy(out.at[pl.ds(reach, reach)], dst.at[pl.ds(own + reach, reach)], corner), *when)
            )
            items.append((copy(occ.at[1], occ_dst.at[bricks + 1], corner), *when))
        return items

    def y_merge(ref, own, width, from_low, from_high, planes):
        first, count = planes
        parts = [from_high[...], from_low[...]]
        if 2 * width < ROWS:
            parts.insert(1, jnp.zeros((count, ROWS - 2 * width, ref.shape[2]), F32))
        ref[first : first + count, own : own + ROWS, :] = jnp.concatenate(parts, axis=1)

    mid_planes, fine_planes = (1, xm + 6), (2, xf + 4)

    def row_prolong(own, extra, index, total, cols, col_own, col_extra, col_index):
        shape = (own + extra, cols)
        fine = logical(iota(shape, 0), own, extra) + own * index
        coarse = logical(iota(shape, 1), col_own, col_extra) + col_own * col_index
        return prolong_matrix(fine, coarse, total, 0)

    def lane_prolong(own, extra, index, total, rows):
        shape = (rows, own + extra)
        fine = logical(iota(shape, 1), own, extra) + own * index
        return prolong_matrix(fine, iota(shape, 0), total, 1)

    def screens(dest, occ_parts, own, extra_rows, bricks_y, lane_matrix, level):
        count = dest.shape[0]
        side = own // bricks_y
        cols = ROWS * len(occ_parts)
        shape = (dest.shape[1], cols)
        brick = lax.div(logical(iota(shape, 0), own, extra_rows) + side, side) - 1
        place = jnp.where(
            brick < 0, ROWS + bricks_y - 1, jnp.where(brick >= bricks_y, 2 * ROWS, brick)
        )
        row_matrix = (place == iota(shape, 1)).astype(BF16)
        for x in range(count):
            flags = jnp.concatenate([part[x] for part in occ_parts], axis=0).astype(BF16)
            wide = mm(flags, lane_matrix).astype(BF16)
            dest[x] = weight[level] * (0.25 + mm(row_matrix, wide))

    def along_y(v):
        n = v.shape[0]
        return pltpu.roll(v, 1, 0), pltpu.roll(v, n - 1, 0)

    def along_z(v):
        n = v.shape[1]
        return pltpu.roll(v, 1, 1), pltpu.roll(v, n - 1, 1)

    lanes_c = (iota((LANES, zc), 0) == lax.div(iota((LANES, zc), 1), zc // bc[2])).astype(BF16)
    arrive(x_coarse)
    halo_mid = x_swap(mb, om, xm, ym, 3, bm[0])
    halo_mid += y_swap(mb, om, xm, ym, 4, 3, m_up, m_dn, m_fu, m_fd, om_l, om_r, bm[0])
    start(halo_mid)
    z_fine = []
    if nz == 2:
        target = {"gz": 1 - iz}
        low = pl.ds(pl.multiple_of((1 - iz) * (zf - LANES), LANES), LANES)
        z_fine.append((copy(
            fb.at[PAD : PAD + xf, 0:yf, low],
            fb.at[PAD : PAD + xf, 0:yf, zf : zf + LANES], target), None, None))
        z_fine.append((copy(
            of.at[1 : 1 + bf[0], :, 0:LANES], of.at[1 : 1 + bf[0], :, LANES : 2 * LANES],
            target), None, None))
    else:
        fb[PAD : PAD + xf, 0:yf, zf:] = jnp.zeros((xf, yf, LANES), F32)
    start(z_fine)
    screens(cs, [oc], yc, 0, bc[1], lanes_c, 0)
    side_c = xc // bc[0]
    shape_c = (yc, zc)
    row_c, lane_c = iota(shape_c, 0), iota(shape_c, 1)

    def sum_c(v, both):
        yu, yd = along_y(v)
        zu, zd = along_z(v)
        total = jnp.where(row_c < yc - 1, yd, 0.0) + jnp.where(lane_c < zc - 1, zd, 0.0)
        if both:
            total = total + jnp.where(row_c > 0, yu, 0.0) + jnp.where(lane_c > 0, zu, 0.0)
        return total

    def coarse_w(p, carry):
        r = cr[p]
        place = xc * ix + p - PAD
        keep = jnp.logical_and(place >= 0, place < xc * nx).astype(F32)
        screen = cs[lax.div(p + (side_c - PAD), side_c)]
        cw[p] = keep * (screen * r - (cr[p - 1] + cr[p + 1] + sum_c(r, True)))
        return carry

    lax.fori_loop(1, xc + 7, coarse_w, 0, unroll=2)

    def coarse_moments(p, acc):
        r, w = cr[p], cw[p]
        screen = cs[lax.div(p + (side_c - PAD), side_c)]
        image = screen * w - 2.0 * (cw[p + 1] + sum_c(w, False))
        return tuple(a + fold_rows(b) for a, b in zip(acc, (r * r, r * w, w * w, w * image)))

    zero = jnp.zeros((ROWS, LANES), F32)

    def spread(value, buf, send, recv, offsets, slot):
        buf[slot] = value
        copies = []
        for k, offset in enumerate(offsets):
            c = pltpu.make_async_remote_copy(
                src_ref=buf.at[slot], dst_ref=buf.at[slot], send_sem=send.at[k],
                recv_sem=recv.at[k], device_id=at(offset), device_id_type=MESH,
            )
            c.start()
            copies.append(c)
        return copies

    def stacked(acc):
        parts = [jnp.sum(a, axis=0, keepdims=True) for a in acc]
        return jnp.concatenate(parts + [jnp.zeros((ROWS - 4, LANES), F32)], axis=0)

    def gathered(copies, buf):
        for c in copies:
            c.wait_recv()
        total = buf[0]
        for k in range(1, buf.shape[0]):
            total = total + buf[k]
        return total

    def solve(total):
        total = jnp.sum(total, axis=1, keepdims=True)
        return coefficients(*[total[k : k + 1] for k in range(4)])

    acc = lax.fori_loop(PAD, PAD + xc, coarse_moments, (zero,) * 4, unroll=2)
    coarse_copies = spread(
        stacked(acc), ac, sc, rc, [(d, 0, 0) for d in range(1, nx)], ix
    )

    arrive(z_fine)
    halo_fine = x_swap(fb, of, xf, yf, 2, bf[0])
    halo_fine += y_swap(fb, of, xf, yf, 2, 2, f_up, f_dn, f_fu, f_fd, of_l, of_r, bf[0])
    start(halo_fine)
    mid_lanes = lane_prolong(zm, 0, 0, zm, zc)
    mid_rows = row_prolong(ym, ROWS, iy, ym * ny, yc, yc, 0, 0)
    ka, kb = solve(gathered(coarse_copies, ac))
    for j in range(xc + 6):
        cx[j] = ka * cr[j + 1] + kb * cw[j + 1]
    out_c[...] = cx[3 : 3 + xc]

    def prolong(src, tz, dst, lane_matrix, row_matrix):
        n, rows, lanes = src.shape
        high, low = split(src[...].reshape(n * rows, lanes))
        tz[...] = (mm(high, lane_matrix) + mm(low, lane_matrix)).reshape(tz.shape)
        for j in range(n):
            high, low = split(tz[j])
            dst[j] = mm(row_matrix, high) + mm(row_matrix, low)

    def interpolate(t, g, own, first, total):
        for p in range(own + 2 * PAD):
            m = p - PAD
            j = m // 2
            beside = min(max(j + (1 if m % 2 else -1) - first, 0), t.shape[0] - 1)
            place = own * ix + m
            keep = jnp.logical_and(place >= 0, place < total).astype(F32)
            g[p] = (0.75 * keep) * t[j - first] + (0.25 * keep) * t[beside]

    def neighbours(v, low_lane, high_lane):
        yu, yd = along_y(v)
        zu, zd = along_z(v)
        if low_lane is not None:
            zu, zd = jnp.where(low_lane, 0.0, zu), jnp.where(high_lane, 0.0, zd)
        return yu + yd + zu + zd

    def later(v, high_lane):
        yd = along_y(v)[1]
        zd = along_z(v)[1]
        if high_lane is not None:
            zd = jnp.where(high_lane, 0.0, zd)
        return yd + zd

    def run_depth(b, g, r, w, s, own, rows, lanes, reach, side, ends, mask):
        low_lane, high_lane = ends
        total_x = own * nx

        def inside(p):
            place = own * ix + p - PAD
            return jnp.logical_and(place >= 0, place < total_x).astype(F32)

        def brick(p):
            return lax.div(p + (side - PAD), side)

        def make_r(p, carry):
            c = g[p]
            value = b[p] - (6.0 + s[brick(p)]) * c
            value = value + (g[p - 1] + g[p + 1]) + neighbours(c, low_lane, high_lane)
            r[p] = value * (mask * inside(p))
            return carry

        lax.fori_loop(PAD - reach, PAD + own + reach, make_r, 0, unroll=4)

        def make_w(p, carry):
            c = r[p]
            value = s[brick(p)] * c - (r[p - 1] + r[p + 1]) - neighbours(c, low_lane, high_lane)
            w[p] = value * (mask * inside(p))
            return carry

        lax.fori_loop(PAD - reach + 1, PAD + own + reach - 1, make_w, 0, unroll=4)

        def moments(p, acc):
            rv, wv = r[p, 0:rows, 0:lanes], w[p, 0:rows, 0:lanes]
            full = w[p]
            image = s[brick(p), 0:rows, 0:lanes] * wv - 2.0 * (
                w[p + 1, 0:rows, 0:lanes] + later(full, high_lane)[0:rows, 0:lanes]
            )
            return tuple(
                a + fold_rows(v) for a, v in zip(acc, (rv * rv, rv * wv, wv * wv, wv * image))
            )

        return lax.fori_loop(PAD, PAD + own, moments, (zero,) * 4, unroll=4)

    prolong(cx, ctz, ct, mid_lanes, mid_rows)
    interpolate(ct, mg, xm, -3, xm * nx)
    arrive(halo_mid)
    left(halo_mid)
    y_merge(mb, ym, 4, m_fu, m_fd, mid_planes)
    lanes_m = (iota((LANES, zm), 0) == lax.div(iota((LANES, zm), 1), zm // bm[2])).astype(BF16)
    screens(ms, [om, om_l, om_r], ym, ROWS, bm[1], lanes_m, 1)
    shape_m = (ym + ROWS, zm)
    row_m = logical(iota(shape_m, 0), ym, ROWS) + ym * iy
    mask_m = jnp.logical_and(row_m >= 0, row_m < ym * ny).astype(F32)
    ends_m = (iota(shape_m, 1) == 0, iota(shape_m, 1) == zm - 1)
    acc = run_depth(mb, mg, mr, mw, ms, xm, ym, zm, 3, xm // bm[0], ends_m, mask_m)
    mid_copies = spread(stacked(acc), am, sm, rm, flat, ix * ny + iy)

    arrive(halo_fine)
    left(halo_fine)
    left(z_fine)
    y_merge(fb, yf, 2, f_fu, f_fd, fine_planes)
    shape_e = (2 * LANES, zf + LANES)
    cell = logical(iota(shape_e, 1), zf, LANES)
    side_z = zf // bf[2]
    brick = lax.div(cell + side_z * LANES, side_z) - LANES
    place = jnp.where(
        brick < 0, LANES + bf[2] + brick, jnp.where(brick >= bf[2], LANES + brick - bf[2], brick)
    )
    lanes_f = (place == iota(shape_e, 0)).astype(BF16)
    screens(fs, [of, of_l, of_r], yf, ROWS, bf[1], lanes_f, 2)
    shape_f = (yf + ROWS, zf + LANES)
    row_f = logical(iota(shape_f, 0), yf, ROWS) + yf * iy
    lane_f = logical(iota(shape_f, 1), zf, LANES) + zf * iz
    mask_f = jnp.logical_and(
        jnp.logical_and(row_f >= 0, row_f < yf * ny), jnp.logical_and(lane_f >= 0, lane_f < zf * nz)
    ).astype(F32)
    fine_lanes = lane_prolong(zf, LANES, iz, zf * nz, zm)
    fine_rows = row_prolong(yf, ROWS, iy, yf * ny, ym + ROWS, ym, ROWS, iy)
    ka, kb = solve(gathered(mid_copies, am))
    for p in range(2, xm + 6):
        value = mg[p] + ka * mr[p] + kb * mw[p]
        mx[p - 2] = value
        if PAD <= p < PAD + xm:
            out_m[p - PAD] = value[0:ym]

    prolong(mx, mtz, mt, fine_lanes, fine_rows)
    interpolate(mt, fg, xf, -2, xf * nx)
    acc = run_depth(fb, fg, fr, fw, fs, xf, yf, zf, 2, xf // bf[0], (None, None), mask_f)
    fine_copies = spread(stacked(acc), af, sf, rf, flat, ix * ny + iy)
    total = gathered(fine_copies, af)
    last_copies = spread(total, ag, sg, rg, across, iz)
    ka, kb = solve(gathered(last_copies, ag))

    def finish(x, carry):
        p = x + PAD
        out_f[x] = (
            fg[p, 0:yf, 0:zf] + ka * fr[p, 0:yf, 0:zf] + kb * fw[p, 0:yf, 0:zf]
        )
        return carry

    lax.fori_loop(0, xf, finish, 0, unroll=4)

    left(x_coarse)
    for c in coarse_copies + mid_copies + fine_copies + last_copies:
        c.wait_send()


def shards(dims, *args):
    nx, ny, nz = dims
    rhs_c, rhs_m, rhs_f, occ_c, occ_m, occ_f, _ = args
    xc, yc, zc = rhs_c.shape
    xm, ym, zm = rhs_m.shape
    xf, yf, zf = rhs_f.shape
    me, fe = (ym + ROWS, zm), (yf + ROWS, zf + LANES)

    def buf(*shape):
        return pltpu.VMEM(shape, F32)

    bm, bf = occ_m.shape[0] + 2, occ_f.shape[0] + 2
    scratch = [
        buf(xc + 8, yc, zc), buf(xc + 8, yc, zc), buf(occ_c.shape[0] + 2, yc, zc),
        buf(xc + 6, yc, zc), buf(xc + 6, yc, zm), buf(xc + 6, *me),
        buf(occ_c.shape[0] + 2, ROWS, LANES),
        buf(xm + 8, *me), buf(xm + 8, *me), buf(xm + 8, *me), buf(xm + 8, *me), buf(bm, *me),
        buf(xm + 4, *me), buf(xm + 4, me[0], fe[1]), buf(xm + 4, *fe),
        buf(bm, ROWS, LANES),
        buf(xm + 6, 4, zm), buf(xm + 6, 4, zm), buf(xm + 6, 4, zm), buf(xm + 6, 4, zm),
        buf(bm, ROWS, LANES), buf(bm, ROWS, LANES),
        buf(xf + 8, *fe), buf(xf + 8, *fe), buf(xf + 8, *fe), buf(xf + 8, *fe), buf(bf, *fe),
        buf(bf, ROWS, 2 * LANES),
        buf(xf + 4, 2, fe[1]), buf(xf + 4, 2, fe[1]), buf(xf + 4, 2, fe[1]), buf(xf + 4, 2, fe[1]),
        buf(bf, ROWS, 2 * LANES), buf(bf, ROWS, 2 * LANES),
        buf(nx, ROWS, LANES), buf(nx * ny, ROWS, LANES), buf(nx * ny, ROWS, LANES),
        buf(nz, ROWS, LANES),
    ]
    for count in (40, nx, nx * ny, nx * ny, nz):
        scratch += [pltpu.SemaphoreType.DMA((count,))] * 2
    vmem = pl.BlockSpec(memory_space=pltpu.VMEM)
    return pl.pallas_call(
        functools.partial(kernel, dims),
        out_shape=[pltpu.VMEM(a.shape, F32) for a in args[:3]],
        in_specs=[vmem] * 6 + [pl.BlockSpec(memory_space=pltpu.SMEM)],
        out_specs=[vmem] * 3,
        scratch_shapes=scratch,
        compiler_params=pltpu.CompilerParams(
            collective_id=0, has_side_effects=True, vmem_limit_bytes=60 * 1024 * 1024
        ),
    )(*args)


def solution(mesh):
    dims = tuple(mesh.shape[axis] for axis in ("gx", "gy", "gz"))
    in_specs = (
        P("gx", None, None), P("gx", "gy", None), P("gx", "gy", "gz"),
        P("gx", None, None), P("gx", "gy", None), P("gx", "gy", "gz"), P(),
    )
    out_specs = (P("gx", None, None), P("gx", "gy", None), P("gx", "gy", "gz"))
    return jax.shard_map(
        functools.partial(shards, dims), mesh=mesh, in_specs=in_specs, out_specs=out_specs,
        check_vma=False,
    )
```

```python
import functools

import jax
import jax.numpy as jnp
from jax import lax
from jax.experimental import pallas as pl
from jax.experimental.pallas import tpu as pltpu
from jax.sharding import PartitionSpec as P

MESH = pl.DeviceIdType.MESH
F32 = jnp.float32
BF16 = jnp.bfloat16
PAD = 4
ROWS = 8
LANES = 128


def iota(shape, dim):
    return lax.broadcasted_iota(jnp.int32, shape, dim)


def logical(index, own, extra):
    if extra == 0:
        return index
    return jnp.where(index < own + extra // 2, index, index - (own + extra))


def prolong_matrix(fine, coarse, total, fine_dim):
    base = lax.shift_right_arithmetic(fine, 1)
    beside = base + 2 * (fine & 1) - 1
    inside = jnp.logical_and(fine >= 0, fine < total)
    value = jnp.where(coarse == base, 0.75, jnp.where(coarse == beside, 0.25, 0.0))
    return jnp.where(inside, value, 0.0).astype(BF16)


def split(values):
    high = values.astype(BF16)
    return high, (values - high.astype(F32)).astype(BF16)


def mm(a, b):
    return jnp.dot(a, b, preferred_element_type=F32)


def fold_rows(values):
    total = values[0:ROWS]
    for row in range(ROWS, values.shape[0], ROWS):
        total = total + values[row : row + ROWS]
    out = total[:, 0:LANES]
    for lane in range(LANES, values.shape[1], LANES):
        out = out + total[:, lane : lane + LANES]
    return out


def coefficients(m0, n1, n2, n3):
    rho = n1 / m0
    spread = n2 - rho * n1
    bent = 6.0 * spread + (n3 - 2.0 * rho * n2 + rho * rho * n1)
    turn = jnp.where(bent > 0.0, jnp.maximum(spread, 0.0) / bent, 0.0)
    first = m0 / ((6.0 + rho) * m0 - jnp.maximum(spread, 0.0) * turn)
    second = -first * turn
    return first - second * rho, second


def kernel(
    dims,
    rhs_c, rhs_m, rhs_f, occ_c, occ_m, occ_f, weight,
    out_c, out_m, out_f,
    cr, cw, cs, cx, ctz, ct, oc,
    mb, mg, mr, mw, ms, mx, mtz, mt, om, m_up, m_dn, m_fu, m_fd, om_l, om_r,
    fb, fg, fr, fw, fs, of, f_up, f_dn, f_fu, f_fd, of_l, of_r,
    ac, am, af, ag, ss, rs, sc, rc, sm, rm, sf, rf, sg, rg,
):
    nx, ny, nz = dims
    ix, iy, iz = lax.axis_index("gx"), lax.axis_index("gy"), lax.axis_index("gz")
    xc, yc, zc = rhs_c.shape
    xm, ym, zm = rhs_m.shape
    xf, yf, zf = rhs_f.shape
    bc, bm, bf = occ_c.shape, occ_m.shape, occ_f.shape
    x_low, x_high = ix > 0, ix < nx - 1
    y_low, y_high = iy > 0, iy < ny - 1

    for ref in (oc, om, of):
        ref[...] = jnp.zeros_like(ref)
    cr[PAD : PAD + xc] = rhs_c[...].astype(F32)
    oc[1 : 1 + bc[0], 0 : bc[1], 0 : bc[2]] = occ_c[...].astype(F32)
    om[1 : 1 + bm[0], 0 : bm[1], 0 : bm[2]] = occ_m[...].astype(F32)
    of[1 : 1 + bf[0], 0 : bf[1], 0 : bf[2]] = occ_f[...].astype(F32)
    mb[PAD : PAD + xm, 0:ym, :] = rhs_m[...].astype(F32)

    def fill_fine(x, carry):
        fb[x + PAD, 0:yf, 0:zf] = rhs_f[x].astype(F32)
        return carry

    lax.fori_loop(0, xf, fill_fine, 0)

    barrier = pltpu.get_barrier_semaphore()
    flat = [(a, b, 0) for a in range(nx) for b in range(ny)][1:]
    across = [(0, 0, c) for c in range(1, nz)]
    peers = flat + across

    def at(offset):
        return (
            lax.rem(ix + offset[0], nx), lax.rem(iy + offset[1], ny), lax.rem(iz + offset[2], nz)
        )

    for offset in peers:
        pl.semaphore_signal(barrier, inc=1, device_id=at(offset), device_id_type=MESH)

    @pl.when(jnp.logical_not(x_low))
    def _():
        cr[0:4] = jnp.zeros((4, yc, zc), F32)
        mb[1:4, 0:ym, :] = jnp.zeros((3, ym, zm), F32)
        fb[2:4, 0:yf, :] = jnp.zeros((2, yf, fb.shape[2]), F32)

    @pl.when(jnp.logical_not(x_high))
    def _():
        cr[PAD + xc : PAD + xc + 4] = jnp.zeros((4, yc, zc), F32)
        mb[PAD + xm : PAD + xm + 3, 0:ym, :] = jnp.zeros((3, ym, zm), F32)
        fb[PAD + xf : PAD + xf + 2, 0:yf, :] = jnp.zeros((2, yf, fb.shape[2]), F32)

    @pl.when(jnp.logical_not(x_low))
    def _():
        for ref, reach in ((m_fu, 3), (m_fd, 3), (f_fu, 2), (f_fd, 2)):
            ref[0:reach] = jnp.zeros((reach,) + tuple(ref.shape[1:]), F32)
        for ref in (om_l, om_r, of_l, of_r):
            ref[0:1] = jnp.zeros((1,) + tuple(ref.shape[1:]), F32)

    @pl.when(jnp.logical_not(x_high))
    def _():
        for ref, reach in ((m_fu, 3), (m_fd, 3), (f_fu, 2), (f_fd, 2)):
            size = ref.shape[0]
            ref[size - reach : size] = jnp.zeros((reach,) + tuple(ref.shape[1:]), F32)
        for ref in (om_l, om_r, of_l, of_r):
            size = ref.shape[0]
            ref[size - 1 : size] = jnp.zeros((1,) + tuple(ref.shape[1:]), F32)

    @pl.when(jnp.logical_not(y_low))
    def _():
        for ref in (m_fu, f_fu, om_l, of_l):
            ref[...] = jnp.zeros_like(ref)

    @pl.when(jnp.logical_not(y_high))
    def _():
        for ref in (m_fd, f_fd, om_r, of_r):
            ref[...] = jnp.zeros_like(ref)

    pl.semaphore_wait(barrier, len(peers))

    used = [0]

    def copy(src, dst, target):
        k = used[0]
        used[0] += 1
        return pltpu.make_async_remote_copy(
            src_ref=src, dst_ref=dst, send_sem=ss.at[k], recv_sem=rs.at[k],
            device_id=target, device_id_type=MESH,
        )

    def start(items):
        for c, can_send, _ in items:
            if can_send is None:
                c.start()
            else:
                pl.when(can_send)(c.start)

    def arrive(items):
        for c, _, can_recv in items:
            if can_recv is None:
                c.wait_recv()
            else:
                pl.when(can_recv)(c.wait_recv)

    def left(items):
        for c, can_send, _ in items:
            if can_send is None:
                c.wait_send()
            else:
                pl.when(can_send)(c.wait_send)

    def x_swap(ref, occ, own, rows, width, bricks):
        items = []
        up, down = {"gx": ix + 1}, {"gx": ix - 1}
        items.append((copy(ref.at[PAD + own - width : PAD + own, 0:rows, :],
                           ref.at[PAD - width : PAD, 0:rows, :], up), x_high, x_low))
        items.append((copy(ref.at[PAD : PAD + width, 0:rows, :],
                           ref.at[PAD + own : PAD + own + width, 0:rows, :], down), x_low, x_high))
        items.append((copy(occ.at[bricks], occ.at[0], up), x_high, x_low))
        items.append((copy(occ.at[1], occ.at[bricks + 1], down), x_low, x_high))
        return items

    x_coarse = x_swap(cr, oc, xc, yc, 4, bc[0])
    start(x_coarse)

    def y_swap(ref, occ, own, rows, width, reach, to_up, to_down, from_low, from_high, occ_l, occ_r, bricks):
        planes, flags = pl.ds(reach, own), pl.ds(1, bricks)
        to_up[planes] = ref[PAD : PAD + own, rows - width : rows, :]
        to_down[planes] = ref[PAD : PAD + own, 0:width, :]
        items = []
        for out, dst, occ_dst, step, can_send, can_recv in (
            (to_up, from_low, occ_l, 1, y_high, y_low), (to_down, from_high, occ_r, -1, y_low, y_high)
        ):
            side = {"gy": iy + step}
            items.append((copy(out.at[planes], dst.at[planes], side), can_send, can_recv))
            items.append((copy(occ.at[flags], occ_dst.at[flags], side), can_send, can_recv))
            corner = {"gx": ix + 1, "gy": iy + step}
            when = (jnp.logical_and(can_send, x_high), jnp.logical_and(can_recv, x_low))
            items.append((copy(out.at[pl.ds(own, reach)], dst.at[pl.ds(0, reach)], corner), *when))
            items.append((copy(occ.at[bricks], occ_dst.at[0], corner), *when))
            corner = {"gx": ix - 1, "gy": iy + step}
            when = (jnp.logical_and(can_send, x_low), jnp.logical_and(can_recv, x_high))
            items.append(
                (copy(out.at[pl.ds(reach, reach)], dst.at[pl.ds(own + reach, reach)], corner), *when)
            )
            items.append((copy(occ.at[1], occ_dst.at[bricks + 1], corner), *when))
        return items

    def y_merge(ref, own, width, from_low, from_high, planes):
        first, count = planes
        parts = [from_high[...], from_low[...]]
        if 2 * width < ROWS:
            parts.insert(1, jnp.zeros((count, ROWS - 2 * width, ref.shape[2]), F32))
        ref[first : first + count, own : own + ROWS, :] = jnp.concatenate(parts, axis=1)

    mid_planes, fine_planes = (1, xm + 6), (2, xf + 4)

    def row_prolong(own, extra, index, total, cols, col_own, col_extra, col_index):
        shape = (own + extra, cols)
        fine = logical(iota(shape, 0), own, extra) + own * index
        coarse = logical(iota(shape, 1), col_own, col_extra) + col_own * col_index
        return prolong_matrix(fine, coarse, total, 0)

    def lane_prolong(own, extra, index, total, rows):
        shape = (rows, own + extra)
        fine = logical(iota(shape, 1), own, extra) + own * index
        return prolong_matrix(fine, iota(shape, 0), total, 1)

    def screens(dest, occ_parts, own, extra_rows, bricks_y, lane_matrix, level):
        count = dest.shape[0]
        side = own // bricks_y
        cols = ROWS * len(occ_parts)
        shape = (dest.shape[1], cols)
        brick = lax.div(logical(iota(shape, 0), own, extra_rows) + side, side) - 1
        place = jnp.where(
            brick < 0, ROWS + bricks_y - 1, jnp.where(brick >= bricks_y, 2 * ROWS, brick)
        )
        row_matrix = (place == iota(shape, 1)).astype(BF16)
        for x in range(count):
            flags = jnp.concatenate([part[x] for part in occ_parts], axis=0).astype(BF16)
            wide = mm(flags, lane_matrix).astype(BF16)
            dest[x] = weight[level] * (0.25 + mm(row_matrix, wide))

    def along_y(v):
        n = v.shape[0]
        return pltpu.roll(v, 1, 0), pltpu.roll(v, n - 1, 0)

    def along_z(v):
        n = v.shape[1]
        return pltpu.roll(v, 1, 1), pltpu.roll(v, n - 1, 1)

    lanes_c = (iota((LANES, zc), 0) == lax.div(iota((LANES, zc), 1), zc // bc[2])).astype(BF16)
    arrive(x_coarse)
    halo_mid = x_swap(mb, om, xm, ym, 3, bm[0])
    halo_mid += y_swap(mb, om, xm, ym, 4, 3, m_up, m_dn, m_fu, m_fd, om_l, om_r, bm[0])
    start(halo_mid)
    z_fine = []
    if nz == 2:
        target = {"gz": 1 - iz}
        low = pl.ds(pl.multiple_of((1 - iz) * (zf - LANES), LANES), LANES)
        z_fine.append((copy(
            fb.at[PAD : PAD + xf, 0:yf, low],
            fb.at[PAD : PAD + xf, 0:yf, zf : zf + LANES], target), None, None))
        z_fine.append((copy(
            of.at[1 : 1 + bf[0], :, 0:LANES], of.at[1 : 1 + bf[0], :, LANES : 2 * LANES],
            target), None, None))
    else:
        fb[PAD : PAD + xf, 0:yf, zf:] = jnp.zeros((xf, yf, LANES), F32)
    start(z_fine)
    screens(cs, [oc], yc, 0, bc[1], lanes_c, 0)
    side_c = xc // bc[0]
    shape_c = (yc, zc)
    row_c, lane_c = iota(shape_c, 0), iota(shape_c, 1)

    def sum_c(v, both):
        yu, yd = along_y(v)
        zu, zd = along_z(v)
        total = jnp.where(row_c < yc - 1, yd, 0.0) + jnp.where(lane_c < zc - 1, zd, 0.0)
        if both:
            total = total + jnp.where(row_c > 0, yu, 0.0) + jnp.where(lane_c > 0, zu, 0.0)
        return total

    def coarse_w(p, carry):
        r = cr[p]
        place = xc * ix + p - PAD
        keep = jnp.logical_and(place >= 0, place < xc * nx).astype(F32)
        screen = cs[lax.div(p + (side_c - PAD), side_c)]
        cw[p] = keep * (screen * r - (cr[p - 1] + cr[p + 1] + sum_c(r, True)))
        return carry

    lax.fori_loop(1, xc + 7, coarse_w, 0, unroll=7)

    def coarse_moments(p, acc):
        r, w = cr[p], cw[p]
        screen = cs[lax.div(p + (side_c - PAD), side_c)]
        image = screen * w - 2.0 * (cw[p + 1] + sum_c(w, False))
        return tuple(a + fold_rows(b) for a, b in zip(acc, (r * r, r * w, w * w, w * image)))

    zero = jnp.zeros((ROWS, LANES), F32)

    def spread(value, buf, send, recv, offsets, slot):
        buf[slot] = value
        copies = []
        for k, offset in enumerate(offsets):
            c = pltpu.make_async_remote_copy(
                src_ref=buf.at[slot], dst_ref=buf.at[slot], send_sem=send.at[k],
                recv_sem=recv.at[k], device_id=at(offset), device_id_type=MESH,
            )
            c.start()
            copies.append(c)
        return copies

    def stacked(acc):
        parts = [jnp.sum(a, axis=0, keepdims=True) for a in acc]
        return jnp.concatenate(parts + [jnp.zeros((ROWS - 4, LANES), F32)], axis=0)

    def gathered(copies, buf):
        for c in copies:
            c.wait_recv()
        total = buf[0]
        for k in range(1, buf.shape[0]):
            total = total + buf[k]
        return total

    def solve(total):
        total = jnp.sum(total, axis=1, keepdims=True)
        return coefficients(*[total[k : k + 1] for k in range(4)])

    acc = lax.fori_loop(PAD, PAD + xc, coarse_moments, (zero,) * 4, unroll=4)
    coarse_copies = spread(
        stacked(acc), ac, sc, rc, [(d, 0, 0) for d in range(1, nx)], ix
    )

    arrive(z_fine)
    halo_fine = x_swap(fb, of, xf, yf, 2, bf[0])
    halo_fine += y_swap(fb, of, xf, yf, 2, 2, f_up, f_dn, f_fu, f_fd, of_l, of_r, bf[0])
    start(halo_fine)
    mid_lanes = lane_prolong(zm, 0, 0, zm, zc)
    mid_rows = row_prolong(ym, ROWS, iy, ym * ny, yc, yc, 0, 0)
    ka, kb = solve(gathered(coarse_copies, ac))
    for j in range(xc + 6):
        cx[j] = ka * cr[j + 1] + kb * cw[j + 1]
    out_c[...] = cx[3 : 3 + xc]

    def prolong(src, tz, dst, lane_matrix, row_matrix):
        n, rows, lanes = src.shape
        high, low = split(src[...].reshape(n * rows, lanes))
        tz[...] = (mm(high, lane_matrix) + mm(low, lane_matrix)).reshape(tz.shape)
        for j in range(n):
            high, low = split(tz[j])
            dst[j] = mm(row_matrix, high) + mm(row_matrix, low)

    def interpolate(t, g, own, first, total):
        for p in range(own + 2 * PAD):
            m = p - PAD
            j = m // 2
            beside = min(max(j + (1 if m % 2 else -1) - first, 0), t.shape[0] - 1)
            place = own * ix + m
            keep = jnp.logical_and(place >= 0, place < total).astype(F32)
            g[p] = (0.75 * keep) * t[j - first] + (0.25 * keep) * t[beside]

    def neighbours(v, low_lane, high_lane):
        yu, yd = along_y(v)
        zu, zd = along_z(v)
        if low_lane is not None:
            zu, zd = jnp.where(low_lane, 0.0, zu), jnp.where(high_lane, 0.0, zd)
        return yu + yd + zu + zd

    def later(v, high_lane):
        yd = along_y(v)[1]
        zd = along_z(v)[1]
        if high_lane is not None:
            zd = jnp.where(high_lane, 0.0, zd)
        return yd + zd

    def run_depth(b, g, r, w, s, own, rows, lanes, reach, side, ends, mask):
        low_lane, high_lane = ends
        total_x = own * nx

        def inside(p):
            place = own * ix + p - PAD
            return jnp.logical_and(place >= 0, place < total_x).astype(F32)

        def brick(p):
            return lax.div(p + (side - PAD), side)

        def make_r(p, carry):
            c = g[p]
            value = b[p] - (6.0 + s[brick(p)]) * c
            value = value + (g[p - 1] + g[p + 1]) + neighbours(c, low_lane, high_lane)
            r[p] = value * (mask * inside(p))
            return carry

        lax.fori_loop(PAD - reach, PAD + own + reach, make_r, 0, unroll=6)

        def make_w(p, carry):
            c = r[p]
            value = s[brick(p)] * c - (r[p - 1] + r[p + 1]) - neighbours(c, low_lane, high_lane)
            w[p] = value * (mask * inside(p))
            return carry

        lax.fori_loop(PAD - reach + 1, PAD + own + 1 + (reach - 2), make_w, 0, unroll=6)

        def moments(p, acc):
            rv, wv = r[p, 0:rows, 0:lanes], w[p, 0:rows, 0:lanes]
            full = w[p]
            image = s[brick(p), 0:rows, 0:lanes] * wv - 2.0 * (
                w[p + 1, 0:rows, 0:lanes] + later(full, high_lane)[0:rows, 0:lanes]
            )
            return tuple(
                a + fold_rows(v) for a, v in zip(acc, (rv * rv, rv * wv, wv * wv, wv * image))
            )

        return lax.fori_loop(PAD, PAD + own, moments, (zero,) * 4, unroll=8)

    prolong(cx, ctz, ct, mid_lanes, mid_rows)
    interpolate(ct, mg, xm, -3, xm * nx)
    arrive(halo_mid)
    left(halo_mid)
    y_merge(mb, ym, 4, m_fu, m_fd, mid_planes)
    lanes_m = (iota((LANES, zm), 0) == lax.div(iota((LANES, zm), 1), zm // bm[2])).astype(BF16)
    screens(ms, [om, om_l, om_r], ym, ROWS, bm[1], lanes_m, 1)
    shape_m = (ym + ROWS, zm)
    row_m = logical(iota(shape_m, 0), ym, ROWS) + ym * iy
    mask_m = jnp.logical_and(row_m >= 0, row_m < ym * ny).astype(F32)
    ends_m = (iota(shape_m, 1) == 0, iota(shape_m, 1) == zm - 1)
    acc = run_depth(mb, mg, mr, mw, ms, xm, ym, zm, 3, xm // bm[0], ends_m, mask_m)
    mid_copies = spread(stacked(acc), am, sm, rm, flat, ix * ny + iy)

    arrive(halo_fine)
    left(halo_fine)
    left(z_fine)
    y_merge(fb, yf, 2, f_fu, f_fd, fine_planes)
    shape_e = (2 * LANES, zf + LANES)
    cell = logical(iota(shape_e, 1), zf, LANES)
    side_z = zf // bf[2]
    brick = lax.div(cell + side_z * LANES, side_z) - LANES
    place = jnp.where(
        brick < 0, LANES + bf[2] + brick, jnp.where(brick >= bf[2], LANES + brick - bf[2], brick)
    )
    lanes_f = (place == iota(shape_e, 0)).astype(BF16)
    screens(fs, [of, of_l, of_r], yf, ROWS, bf[1], lanes_f, 2)
    shape_f = (yf + ROWS, zf + LANES)
    row_f = logical(iota(shape_f, 0), yf, ROWS) + yf * iy
    lane_f = logical(iota(shape_f, 1), zf, LANES) + zf * iz
    mask_f = jnp.logical_and(
        jnp.logical_and(row_f >= 0, row_f < yf * ny), jnp.logical_and(lane_f >= 0, lane_f < zf * nz)
    ).astype(F32)
    fine_lanes = lane_prolong(zf, LANES, iz, zf * nz, zm)
    fine_rows = row_prolong(yf, ROWS, iy, yf * ny, ym + ROWS, ym, ROWS, iy)
    ka, kb = solve(gathered(mid_copies, am))
    for p in range(2, xm + 6):
        value = mg[p] + ka * mr[p] + kb * mw[p]
        mx[p - 2] = value
        if PAD <= p < PAD + xm:
            out_m[p - PAD] = value[0:ym]

    prolong(mx, mtz, mt, fine_lanes, fine_rows)
    interpolate(mt, fg, xf, -2, xf * nx)
    acc = run_depth(fb, fg, fr, fw, fs, xf, yf, zf, 2, xf // bf[0], (None, None), mask_f)
    fine_copies = spread(stacked(acc), af, sf, rf, flat, ix * ny + iy)
    total = gathered(fine_copies, af)
    last_copies = spread(total, ag, sg, rg, across, iz)
    ka, kb = solve(gathered(last_copies, ag))

    def finish(x, carry):
        p = x + PAD
        out_f[x] = (
            fg[p, 0:yf, 0:zf] + ka * fr[p, 0:yf, 0:zf] + kb * fw[p, 0:yf, 0:zf]
        )
        return carry

    lax.fori_loop(0, xf, finish, 0, unroll=4)

    left(x_coarse)
    for c in coarse_copies + mid_copies + fine_copies + last_copies:
        c.wait_send()


def shards(dims, *args):
    nx, ny, nz = dims
    rhs_c, rhs_m, rhs_f, occ_c, occ_m, occ_f, _ = args
    xc, yc, zc = rhs_c.shape
    xm, ym, zm = rhs_m.shape
    xf, yf, zf = rhs_f.shape
    me, fe = (ym + ROWS, zm), (yf + ROWS, zf + LANES)

    def buf(*shape):
        return pltpu.VMEM(shape, F32)

    bm, bf = occ_m.shape[0] + 2, occ_f.shape[0] + 2
    scratch = [
        buf(xc + 8, yc, zc), buf(xc + 8, yc, zc), buf(occ_c.shape[0] + 2, yc, zc),
        buf(xc + 6, yc, zc), buf(xc + 6, yc, zm), buf(xc + 6, *me),
        buf(occ_c.shape[0] + 2, ROWS, LANES),
        buf(xm + 8, *me), buf(xm + 8, *me), buf(xm + 8, *me), buf(xm + 8, *me), buf(bm, *me),
        buf(xm + 4, *me), buf(xm + 4, me[0], fe[1]), buf(xm + 4, *fe),
        buf(bm, ROWS, LANES),
        buf(xm + 6, 4, zm), buf(xm + 6, 4, zm), buf(xm + 6, 4, zm), buf(xm + 6, 4, zm),
        buf(bm, ROWS, LANES), buf(bm, ROWS, LANES),
        buf(xf + 8, *fe), buf(xf + 8, *fe), buf(xf + 8, *fe), buf(xf + 8, *fe), buf(bf, *fe),
        buf(bf, ROWS, 2 * LANES),
        buf(xf + 4, 2, fe[1]), buf(xf + 4, 2, fe[1]), buf(xf + 4, 2, fe[1]), buf(xf + 4, 2, fe[1]),
        buf(bf, ROWS, 2 * LANES), buf(bf, ROWS, 2 * LANES),
        buf(nx, ROWS, LANES), buf(nx * ny, ROWS, LANES), buf(nx * ny, ROWS, LANES),
        buf(nz, ROWS, LANES),
    ]
    for count in (40, nx, nx * ny, nx * ny, nz):
        scratch += [pltpu.SemaphoreType.DMA((count,))] * 2
    vmem = pl.BlockSpec(memory_space=pltpu.VMEM)
    return pl.pallas_call(
        functools.partial(kernel, dims),
        out_shape=[pltpu.VMEM(a.shape, F32) for a in args[:3]],
        in_specs=[vmem] * 6 + [pl.BlockSpec(memory_space=pltpu.SMEM)],
        out_specs=[vmem] * 3,
        scratch_shapes=scratch,
        compiler_params=pltpu.CompilerParams(
            collective_id=0, has_side_effects=True, vmem_limit_bytes=60 * 1024 * 1024
        ),
    )(*args)


def solution(mesh):
    dims = tuple(mesh.shape[axis] for axis in ("gx", "gy", "gz"))
    in_specs = (
        P("gx", None, None), P("gx", "gy", None), P("gx", "gy", "gz"),
        P("gx", None, None), P("gx", "gy", None), P("gx", "gy", "gz"), P(),
    )
    out_specs = (P("gx", None, None), P("gx", "gy", None), P("gx", "gy", "gz"))
    return jax.shard_map(
        functools.partial(shards, dims), mesh=mesh, in_specs=in_specs, out_specs=out_specs,
        check_vma=False,
    )
```
